32 devices in a mesh: row: 8 (over y, x, core), col: 4 (over z).
Axes of the slice: x: 2, y: 2, z: 4, core: 2. Of those that a mesh axis runs over, the one named last changes fastest.
Arguments:
- columns: float32 [4096, 8192], P('col', 'row'), may hold values from -64 to 64
- block_order: int32 [64], P('col'), may hold values from 0 to 63, as said below
Outputs:
- rotated: float32 [4096, 8192], P('col', 'row')
The draws below stay inside these ranges and needn't reach their ends.
Inputs may be any that keep to these rules, and one draw needn't show every extreme that they name: block_order is a permutation of 0 .. 63 in which slots c * 16 to (c + 1) * 16 - 1 name blocks c * 16 to (c + 1) * 16 - 1.
All inputs are finite; a program needn't handle non-finite values.
Results may differ from the reference program's by a relative error of at most 0.00055.
Values sent between devices are 32-bit elements; how exact they have to be, the bound alone decides.
A program may use at most 64 MiB of HBM per device.

```python
import math
import jax
import jax.numpy as jnp
from jax import lax

BLOCK = 64
STEPS = 4
BLOCKS_DEV = 16
N = 4096
M = 8192
BLOCKS = 64


def draw_columns(key, part):
    keys = jax.random.split(key, 4)
    gain_rows = 1.0 + 2.0 * jnp.arange(M, dtype=jnp.float32) / M
    loadings = jax.random.truncated_normal(keys[2], -3.0, 3.0, (N,), jnp.float32)
    noise = jax.random.truncated_normal(keys[0], -4.0, 4.0, (N, M), jnp.float32)
    scales = jnp.exp(jax.random.uniform(keys[1], (N,), jnp.float32, math.log(0.3), math.log(3.0)))
    common = jax.random.truncated_normal(keys[3], -3.0, 3.0, (M,), jnp.float32)
    return noise * scales[:, None] + loadings[:, None] * (common * gain_rows)[None, :]


def draw_block_order(key, part):
    groups = BLOCKS // BLOCKS_DEV
    scores = jax.random.randint(key, (groups, BLOCKS_DEV), 0, 1 << 20) * BLOCKS_DEV + jnp.arange(BLOCKS_DEV, dtype=jnp.int32)[None, :]
    shuffled = jnp.argsort(scores, axis=1, stable=True).astype(jnp.int32)
    return (shuffled + (jnp.arange(groups, dtype=jnp.int32) * BLOCKS_DEV)[:, None]).reshape(-1)


def setup_inputs(seed: int = 0) -> dict:
    splits = jax.random.split(jax.random.key(seed), 3)
    return {
        "columns": draw_columns(jax.random.fold_in(splits[2], 71), 0),
        "block_order": draw_block_order(jax.random.fold_in(splits[2], 71), 0),
    }


def cayley_turn(cross_sum, col_norms):
    highest = lax.Precision.HIGHEST
    top_norms = col_norms[:, :BLOCK][:, :, None]
    bottom_norms = col_norms[:, BLOCK:][:, None, :]
    spread = bottom_norms - top_norms
    radius = jnp.sqrt(spread * spread + 4.0 * cross_sum * cross_sum)
    scale_term = (top_norms + bottom_norms) / BLOCK
    coupling = 2.0 * cross_sum * spread / (spread * spread + 4.0 * cross_sum * cross_sum + jnp.abs(spread) * radius + scale_term * scale_term)
    identity = jnp.eye(BLOCK, dtype=jnp.float32)
    left_system = identity + jnp.einsum('pij,pkj->pik', coupling, coupling, precision=highest)
    right_system = identity + jnp.einsum('pji,pjk->pik', coupling, coupling, precision=highest)
    left_factor = jnp.linalg.cholesky(left_system)
    right_factor = jnp.linalg.cholesky(right_system)
    identities = jnp.broadcast_to(identity, coupling.shape)
    upper_half = jnp.concatenate([identities, coupling], axis=2)
    lower_half = jnp.concatenate([-jnp.transpose(coupling, (0, 2, 1)), identities], axis=2)

    def solve_one(factor, target):
        return jax.scipy.linalg.cho_solve((factor, True), target)
    upper_solved = jax.vmap(solve_one)(left_factor, upper_half)
    lower_solved = jax.vmap(solve_one)(right_factor, lower_half)
    solved = jnp.concatenate([upper_solved, lower_solved], axis=1)
    plus_skew = jnp.concatenate([upper_half, lower_half], axis=1)
    return jnp.einsum('pij,pjk->pik', plus_skew, solved, precision=highest)

def reference(columns, block_order):
    highest = lax.Precision.HIGHEST
    width, length = columns.shape
    count = width // BLOCK
    blocks = jnp.take(columns.reshape(count, BLOCK, length), block_order.astype(jnp.int32), axis=0)
    blocks = blocks.reshape(count // 2, 2 * BLOCK, length)
    for sweep_step in range(STEPS):
        gram_sum = jnp.einsum('pim,pjm->pij', blocks, blocks, precision=highest)
        col_norms = jnp.diagonal(gram_sum, axis1=1, axis2=2)
        cross_sum = gram_sum[:, :BLOCK, BLOCK:]
        turn_matrix = cayley_turn(cross_sum, col_norms)
        turned = jnp.einsum('pij,pim->pjm', turn_matrix, blocks, precision=highest)
        top_blocks = turned[:, :BLOCK]
        bottom_blocks = turned[:, BLOCK:]
        new_tops = jnp.concatenate([top_blocks[:1], bottom_blocks[:1], top_blocks[1:-1]], axis=0)
        new_bottoms = jnp.concatenate([bottom_blocks[1:], top_blocks[-1:]], axis=0)
        blocks = jnp.concatenate([new_tops, new_bottoms], axis=1)
    return blocks.reshape(width, length)
```

```python
import functools

import jax
import jax.numpy as jnp
from jax import lax
from jax.experimental import pallas as pl
from jax.experimental.pallas import tpu as pltpu
from jax.sharding import PartitionSpec as P

BLOCK = 64
PAIR = 2 * BLOCK
STEPS = 4
HALF = BLOCK // 2
PACKED = HALF + 8
UPPER = 1.0 + BLOCK * BLOCK * 0.0905
HIGHEST = lax.Precision.HIGHEST


def mm(a, b):
    return jnp.dot(a, b, precision=HIGHEST, preferred_element_type=jnp.float32)


def inverse(coupling, coupling_t, eye):
    system = eye + mm(coupling, coupling_t)
    low = 2.0 / (1.0 + UPPER)
    y = system * low
    reach = low * (2.0 - low)
    scale = 2.0 / (1.0 + reach)
    z = 2.0 * eye - y
    x = (scale * low) * z
    y = scale * mm(y, z)
    low = scale * reach
    while low < 0.99:
        z = 2.0 * eye - y
        reach = low * (2.0 - low)
        scale = 2.0 / (1.0 + reach)
        stacked = scale * mm(jnp.concatenate([x, y], axis=0), z)
        x, y = stacked[:BLOCK], stacked[BLOCK:]
        low = scale * reach
    x = x + mm(x, eye - mm(system, x))
    x = x + mm(x, eye - x - mm(coupling, mm(coupling_t, x)))
    return 0.5 * (x + x.T)


def turn_transposed(total):
    cross = jnp.concatenate([total[:HALF, :BLOCK], total[:HALF, BLOCK:]], axis=0)
    norms = total[HALF : HALF + 1, :]
    rows = lax.broadcasted_iota(jnp.int32, (BLOCK, BLOCK), 0)
    cols = lax.broadcasted_iota(jnp.int32, (BLOCK, BLOCK), 1)
    eye = jnp.where(rows == cols, 1.0, 0.0).astype(jnp.float32)
    top_norms = jnp.sum(jnp.where(rows == cols, norms[:, :BLOCK], 0.0), axis=1, keepdims=True)
    bottom_norms = norms[:, BLOCK:]
    spread = bottom_norms - top_norms
    square = spread * spread + 4.0 * cross * cross
    radius = jnp.sqrt(square)
    scale_term = (top_norms + bottom_norms) / BLOCK
    coupling = 2.0 * cross * spread / (square + jnp.abs(spread) * radius + scale_term * scale_term)
    coupling_t = coupling.T
    x = inverse(coupling, coupling_t, eye)
    lower = 2.0 * mm(coupling_t, x)
    upper = lower.T
    corner = eye - mm(lower, coupling)
    return jnp.concatenate(
        [jnp.concatenate([2.0 * x - eye, -upper], axis=1), jnp.concatenate([lower, corner], axis=1)], axis=0
    )


def kernel(rows, cols, pairs, order_ref, columns_ref, out_ref, x, grams, parts, turns, edges,
           gram_send, gram_recv, turn_send, turn_recv, pass_send, edge_send, edge_recv, out_sem):
    me = lax.axis_index("row")
    position = lax.axis_index("col")
    core = lax.rem(me, 2)
    chip = lax.div(me, 2)
    partner = me + 1 - 2 * core
    has_left = position > 0
    has_right = position < cols - 1
    last = pairs - 1
    width = pairs * PAIR

    barrier = pltpu.get_barrier_semaphore()

    def greet(other, carry):
        @pl.when(other != me)
        def _():
            pl.semaphore_signal(barrier, inc=1, device_id={"row": other})
        return carry

    lax.fori_loop(0, rows, greet, 0)

    @pl.when(has_left)
    def _():
        pl.semaphore_signal(barrier, inc=1, device_id={"col": position - 1})

    @pl.when(has_right)
    def _():
        pl.semaphore_signal(barrier, inc=1, device_id={"col": position + 1})

    def fill(slot, carry):
        source = lax.rem(order_ref[slot], 2 * pairs)
        x[0, pl.ds(pl.multiple_of(slot * BLOCK, BLOCK), BLOCK), :] = columns_ref[source]
        return carry

    lax.fori_loop(0, 2 * pairs, fill, 0)

    greeted = rows - 1 + has_left.astype(jnp.int32) + has_right.astype(jnp.int32)
    pl.semaphore_wait(barrier, greeted)

    def gram_copy(pair):
        return pltpu.make_async_remote_copy(
            src_ref=grams.at[pair], dst_ref=parts.at[me], send_sem=gram_send.at[pair], recv_sem=gram_recv.at[me],
            device_id={"row": pair},
        )

    def gram_arrival(source):
        return pltpu.make_async_remote_copy(
            src_ref=parts.at[source], dst_ref=parts.at[source], send_sem=gram_send.at[0],
            recv_sem=gram_recv.at[source], device_id={"row": partner},
        )

    def turn_copy(other):
        target = jnp.where(other == chip, partner, 2 * other + core)
        return pltpu.make_async_remote_copy(
            src_ref=turns.at[me], dst_ref=turns.at[me], send_sem=turn_send.at[other], recv_sem=turn_recv.at[me],
            device_id={"row": target},
        )

    def pass_copy(pair):
        return pltpu.make_async_remote_copy(
            src_ref=turns.at[pair], dst_ref=turns.at[pair], send_sem=pass_send.at[pair], recv_sem=turn_recv.at[pair],
            device_id={"row": partner},
        )

    def edge_left(after):
        return pltpu.make_async_remote_copy(
            src_ref=edges.at[0], dst_ref=x.at[after, pl.ds(last * PAIR + BLOCK, BLOCK)], send_sem=edge_send.at[0],
            recv_sem=edge_recv.at[after, 0], device_id={"col": position - 1},
        )

    def edge_right(after):
        return pltpu.make_async_remote_copy(
            src_ref=edges.at[1], dst_ref=x.at[after, pl.ds(0, BLOCK)], send_sem=edge_send.at[1],
            recv_sem=edge_recv.at[after, 1], device_id={"col": position + 1},
        )

    def wait_edges(now):
        @pl.when(has_left)
        def _():
            edge_right(now).wait_recv()

        @pl.when(has_right)
        def _():
            edge_left(now).wait_recv()

    def take_gram(pair, now):
        base = pl.multiple_of(pair * PAIR, PAIR)
        block = x[now, pl.ds(base, PAIR), :]
        cross = lax.dot_general(
            block[:BLOCK], block[BLOCK:], (((1,), (1,)), ((), ())), precision=HIGHEST,
            preferred_element_type=jnp.float32,
        )
        squares = block * block
        partial = squares[:, :128]
        for lane in range(1, squares.shape[1] // 128):
            partial = partial + squares[:, lane * 128 : (lane + 1) * 128]
        norms = jnp.sum(partial.T, axis=0, keepdims=True)
        grams[pair, :HALF, :] = jnp.concatenate([cross[:HALF], cross[HALF:]], axis=1)
        grams[pair, HALF:, :] = jnp.broadcast_to(norms, (8, PAIR))

        @pl.when(pair != me)
        def _():
            gram_copy(pair).start()

    def own():
        def gather(source, carry):
            @pl.when(source != me)
            def _():
                gram_arrival(source).wait_recv()
            return carry

        lax.fori_loop(0, rows, gather, 0)
        total = grams[me]
        for source in range(rows):
            total = total + jnp.where(source == me, 0.0, parts[source])
        turns[me] = turn_transposed(total)

        def spread_out(other, carry):
            turn_copy(other).start()
            return carry

        lax.fori_loop(0, rows // 2, spread_out, 0)

    def take_turn(pair):
        @pl.when(pair != me)
        def _():
            pass_copy(pair).wait_recv()

            @pl.when(lax.rem(pair, 2) == core)
            def _():
                pass_copy(pair).start()

    def apply(pair, now):
        base = pl.multiple_of(pair * PAIR, PAIR)
        return mm(turns[pair], x[now, pl.ds(base, PAIR), :])

    def step(index, carry):
        now = lax.rem(index, 2)
        after = 1 - now

        def inner_gram(pair, carry):
            take_gram(pair, now)
            return carry

        lax.fori_loop(1, last, inner_gram, 0)
        inner_owner = jnp.logical_and(me > 0, me < last)
        edge_owner = jnp.logical_or(me == 0, me == last)

        @pl.when(inner_owner)
        def _():
            own()

        @pl.when(index > 0)
        def _():
            wait_edges(now)

        def edge_gram(which, carry):
            take_gram(which * last, now)
            return carry

        lax.fori_loop(0, 2, edge_gram, 0)

        @pl.when(edge_owner)
        def _():
            own()

        def inner_apply(pair, carry):
            take_turn(pair)
            turned = apply(pair, now)
            x[after, pl.ds(pl.multiple_of((pair + 1) * PAIR, PAIR), BLOCK), :] = turned[:BLOCK]
            x[after, pl.ds(pl.multiple_of((pair - 1) * PAIR + BLOCK, BLOCK), BLOCK), :] = turned[BLOCK:]
            return carry

        lax.fori_loop(1, last, inner_apply, 0)

        @pl.when(jnp.logical_and(index > 0, has_left))
        def _():
            edge_left(after).wait_send()

        take_turn(0)
        turned = apply(0, now)
        x[after, pl.ds(pl.multiple_of(jnp.where(has_left, PAIR, 0), BLOCK), BLOCK), :] = turned[:BLOCK]

        @pl.when(has_left)
        def _():
            edges[0] = turned[BLOCK:]
            edge_left(after).start()

        @pl.when(jnp.logical_not(has_left))
        def _():
            x[after, pl.ds(PAIR, BLOCK), :] = turned[BLOCK:]

        @pl.when(jnp.logical_and(index > 0, has_right))
        def _():
            edge_right(after).wait_send()

        take_turn(last)
        turned_last = apply(last, now)
        x[after, pl.ds((last - 1) * PAIR + BLOCK, BLOCK), :] = turned_last[BLOCK:]

        @pl.when(has_right)
        def _():
            edges[1] = turned_last[:BLOCK]
            edge_right(after).start()

        @pl.when(jnp.logical_not(has_right))
        def _():
            x[after, pl.ds(last * PAIR + BLOCK, BLOCK), :] = turned_last[:BLOCK]

        def settle(pair, carry):
            @pl.when(pair != me)
            def _():
                gram_copy(pair).wait_send()

                @pl.when(lax.rem(pair, 2) == core)
                def _():
                    pass_copy(pair).wait_send()
            return carry

        lax.fori_loop(0, pairs, settle, 0)

        @pl.when(me < pairs)
        def _():
            def settle_turn(other, carry):
                turn_copy(other).wait_send()
                return carry

            lax.fori_loop(0, rows // 2, settle_turn, 0)

        return carry

    lax.fori_loop(0, STEPS, step, 0)
    final = STEPS % 2

    def out_copy(start, size, which):
        return pltpu.make_async_copy(
            x.at[final, pl.ds(start, size)], out_ref.at[pl.ds(start, size)], out_sem.at[which]
        )

    middle = out_copy(BLOCK, width - PAIR, 0)
    middle.start()
    wait_edges(final)
    first = out_copy(0, BLOCK, 1)
    first.start()
    ending = out_copy(width - BLOCK, BLOCK, 2)
    ending.start()

    @pl.when(has_left)
    def _():
        edge_left(final).wait_send()

    @pl.when(has_right)
    def _():
        edge_right(final).wait_send()

    middle.wait()
    first.wait()
    ending.wait()


def solution(mesh):
    rows, cols = mesh.shape["row"], mesh.shape["col"]

    def local(columns, block_order):
        width, length = columns.shape
        pairs = width // PAIR
        assert 3 <= pairs <= rows and rows % 2 == 0
        dma = pltpu.SemaphoreType.DMA
        return pl.pallas_call(
            functools.partial(kernel, rows, cols, pairs),
            out_shape=jax.ShapeDtypeStruct((width, length), jnp.float32),
            in_specs=[pl.BlockSpec(memory_space=pltpu.SMEM), pl.BlockSpec(memory_space=pltpu.VMEM)],
            out_specs=pl.BlockSpec(memory_space=pl.ANY),
            scratch_shapes=[
                pltpu.VMEM((2, width, length), jnp.float32),
                pltpu.VMEM((pairs, PACKED, PAIR), jnp.float32),
                pltpu.VMEM((rows, PACKED, PAIR), jnp.float32),
                pltpu.VMEM((pairs, PAIR, PAIR), jnp.float32),
                pltpu.VMEM((2, BLOCK, length), jnp.float32),
                dma((pairs,)),
                dma((rows,)),
                dma((rows // 2,)),
                dma((pairs,)),
                dma((pairs,)),
                dma((2,)),
                dma((2, 2)),
                dma((3,)),
            ],
            compiler_params=pltpu.CompilerParams(
                collective_id=0, has_side_effects=True, vmem_limit_bytes=56 * 1024 * 1024
            ),
        )(block_order, columns.reshape(2 * pairs, BLOCK, length))

    placed = (P("col", "row"), P("col"))
    return jax.shard_map(local, mesh=mesh, in_specs=placed, out_specs=P("col", "row"), check_vma=False)
```

```python
import functools

import jax
import jax.numpy as jnp
from jax import lax
from jax.experimental import pallas as pl
from jax.experimental.pallas import tpu as pltpu
from jax.sharding import PartitionSpec as P

BLOCK = 64
PAIR = 2 * BLOCK
STEPS = 4
HALF = BLOCK // 2
PACKED = HALF + 8
UPPER = 1.0 + BLOCK * BLOCK * 0.0905
HIGHEST = lax.Precision.HIGHEST


def split(a):
    high = a.astype(jnp.bfloat16)
    rest = a - high.astype(jnp.float32)
    middle = rest.astype(jnp.bfloat16)
    return high, middle, (rest - middle.astype(jnp.float32)).astype(jnp.bfloat16)


def chain(lefts, rights):
    return jnp.dot(
        jnp.concatenate(lefts, axis=1), jnp.concatenate(rights, axis=0), preferred_element_type=jnp.float32
    )


def mm3(a, b):
    (ah, am, _), (bh, bm, _) = split(a), split(b)
    return chain([ah, am, ah], [bh, bh, bm])


def mm4(a, b):
    (ah, am, al), (bh, bm, _) = split(a), split(b)
    return chain([al, am, ah, ah], [bh, bh, bm, bh])


def mm(a, b):
    (ah, am, al), (bh, bm, bl) = split(a), split(b)
    return chain([am, al, ah, ah, am, ah], [bm, bh, bl, bm, bh, bh])


def inverse(coupling, coupling_t, eye):
    system = eye + mm3(coupling, coupling_t)
    low = 2.0 / (1.0 + UPPER)
    y = system * low
    reach = low * (2.0 - low)
    scale = 2.0 / (1.0 + reach)
    z = 2.0 * eye - y
    x = (scale * low) * z
    y = scale * mm3(y, z)
    low = scale * reach
    while low < 0.99:
        z = 2.0 * eye - y
        reach = low * (2.0 - low)
        scale = 2.0 / (1.0 + reach)
        stacked = scale * mm3(jnp.concatenate([x, y], axis=0), z)
        x, y = stacked[:BLOCK], stacked[BLOCK:]
        low = scale * reach
    x = x + mm3(x, eye - mm3(system, x))
    product = mm(coupling_t, x)
    residual = eye - x - mm(coupling, product)
    stacked = jnp.concatenate([x, product], axis=0)
    stacked = stacked + mm3(stacked, residual)
    return stacked[:BLOCK], stacked[BLOCK:]


def turn_transposed(total):
    cross = jnp.concatenate([total[:HALF, :BLOCK], total[:HALF, BLOCK:]], axis=0)
    norms = total[HALF : HALF + 1, :]
    rows = lax.broadcasted_iota(jnp.int32, (BLOCK, BLOCK), 0)
    cols = lax.broadcasted_iota(jnp.int32, (BLOCK, BLOCK), 1)
    eye = jnp.where(rows == cols, 1.0, 0.0).astype(jnp.float32)
    top_norms = jnp.sum(jnp.where(rows == cols, norms[:, :BLOCK], 0.0), axis=1, keepdims=True)
    bottom_norms = norms[:, BLOCK:]
    spread = bottom_norms - top_norms
    square = spread * spread + 4.0 * cross * cross
    radius = jnp.sqrt(square)
    scale_term = (top_norms + bottom_norms) / BLOCK
    coupling = 2.0 * cross * spread / (square + jnp.abs(spread) * radius + scale_term * scale_term)
    coupling_t = coupling.T
    x, product = inverse(coupling, coupling_t, eye)
    lower = 2.0 * product
    corner = eye - mm(lower, coupling)
    diagonal = jnp.sum(jnp.where(rows == cols, corner, 0.0), axis=0, keepdims=True)
    mixed = jnp.where(rows <= cols, 2.0 * x - eye, corner)
    body = jnp.concatenate([mixed, -lower.T], axis=1)
    foot = jnp.broadcast_to(jnp.concatenate([diagonal, diagonal], axis=1), (8, PAIR))
    return jnp.concatenate([body, foot], axis=0)


def unpacked(packed):
    rows = lax.broadcasted_iota(jnp.int32, (BLOCK, BLOCK), 0)
    cols = lax.broadcasted_iota(jnp.int32, (BLOCK, BLOCK), 1)
    mixed, upper = packed[:BLOCK, :BLOCK], packed[:BLOCK, BLOCK:]
    flipped = mixed.T
    corner = jnp.where(rows == cols, packed[BLOCK : BLOCK + 1, :BLOCK], jnp.where(rows > cols, mixed, flipped))
    return jnp.concatenate(
        [
            jnp.concatenate([jnp.where(rows <= cols, mixed, flipped), upper], axis=1),
            jnp.concatenate([-upper.T, corner], axis=1),
        ],
        axis=0,
    )


def kernel(rows, cols, pairs, order_ref, columns_ref, out_ref, x, grams, parts, turns, edges,
           gram_send, gram_recv, turn_send, turn_recv, pass_send, edge_send, edge_recv, out_sem):
    me = lax.axis_index("row")
    position = lax.axis_index("col")
    core = lax.rem(me, 2)
    chip = lax.div(me, 2)
    partner = me + 1 - 2 * core
    has_left = position > 0
    has_right = position < cols - 1
    last = pairs - 1
    width = pairs * PAIR

    barrier = pltpu.get_barrier_semaphore()

    def greet(other, carry):
        @pl.when(other != me)
        def _():
            pl.semaphore_signal(barrier, inc=1, device_id={"row": other})
        return carry

    lax.fori_loop(0, rows, greet, 0)

    @pl.when(has_left)
    def _():
        pl.semaphore_signal(barrier, inc=1, device_id={"col": position - 1})

    @pl.when(has_right)
    def _():
        pl.semaphore_signal(barrier, inc=1, device_id={"col": position + 1})

    def fill(slot, carry):
        source = lax.rem(order_ref[slot], 2 * pairs)
        x[0, pl.ds(pl.multiple_of(slot * BLOCK, BLOCK), BLOCK), :] = columns_ref[source]
        return carry

    lax.fori_loop(0, 2 * pairs, fill, 0)

    greeted = rows - 1 + has_left.astype(jnp.int32) + has_right.astype(jnp.int32)
    pl.semaphore_wait(barrier, greeted)

    def gram_copy(pair):
        return pltpu.make_async_remote_copy(
            src_ref=grams.at[pair], dst_ref=parts.at[me], send_sem=gram_send.at[pair], recv_sem=gram_recv.at[me],
            device_id={"row": pair},
        )

    def gram_arrival(source):
        return pltpu.make_async_remote_copy(
            src_ref=parts.at[source], dst_ref=parts.at[source], send_sem=gram_send.at[0],
            recv_sem=gram_recv.at[source], device_id={"row": partner},
        )

    def turn_copy(other):
        target = jnp.where(other == chip, partner, 2 * other + core)
        return pltpu.make_async_remote_copy(
            src_ref=turns.at[me], dst_ref=turns.at[me], send_sem=turn_send.at[other], recv_sem=turn_recv.at[me],
            device_id={"row": target},
        )

    def pass_copy(pair):
        return pltpu.make_async_remote_copy(
            src_ref=turns.at[pair], dst_ref=turns.at[pair], send_sem=pass_send.at[pair], recv_sem=turn_recv.at[pair],
            device_id={"row": partner},
        )

    def edge_left(after):
        return pltpu.make_async_remote_copy(
            src_ref=edges.at[0], dst_ref=x.at[after, pl.ds(last * PAIR + BLOCK, BLOCK)], send_sem=edge_send.at[0],
            recv_sem=edge_recv.at[after, 0], device_id={"col": position - 1},
        )

    def edge_right(after):
        return pltpu.make_async_remote_copy(
            src_ref=edges.at[1], dst_ref=x.at[after, pl.ds(0, BLOCK)], send_sem=edge_send.at[1],
            recv_sem=edge_recv.at[after, 1], device_id={"col": position + 1},
        )

    def wait_edges(now):
        @pl.when(has_left)
        def _():
            edge_right(now).wait_recv()

        @pl.when(has_right)
        def _():
            edge_left(now).wait_recv()

    def take_gram(pair, now):
        base = pl.multiple_of(pair * PAIR, PAIR)
        block = x[now, pl.ds(base, PAIR), :]
        cross = lax.dot_general(
            block[:BLOCK], block[BLOCK:], (((1,), (1,)), ((), ())), precision=HIGHEST,
            preferred_element_type=jnp.float32,
        )
        squares = block * block
        partial = squares[:, :128]
        for lane in range(1, squares.shape[1] // 128):
            partial = partial + squares[:, lane * 128 : (lane + 1) * 128]
        norms = jnp.sum(partial.T, axis=0, keepdims=True)
        grams[pair, :HALF, :] = jnp.concatenate([cross[:HALF], cross[HALF:]], axis=1)
        grams[pair, HALF:, :] = jnp.broadcast_to(norms, (8, PAIR))

        @pl.when(pair != me)
        def _():
            gram_copy(pair).start()

    def own():
        def gather(source, carry):
            @pl.when(source != me)
            def _():
                gram_arrival(source).wait_recv()
            return carry

        lax.fori_loop(0, rows, gather, 0)
        total = grams[me]
        for source in range(rows):
            total = total + jnp.where(source == me, 0.0, parts[source])
        turns[me] = turn_transposed(total)

        def spread_out(other, carry):
            turn_copy(other).start()
            return carry

        lax.fori_loop(0, rows // 2, spread_out, 0)

    def take_turn(pair):
        @pl.when(pair != me)
        def _():
            pass_copy(pair).wait_recv()

            @pl.when(lax.rem(pair, 2) == core)
            def _():
                pass_copy(pair).start()

    def apply(pair, now):
        base = pl.multiple_of(pair * PAIR, PAIR)
        return mm4(unpacked(turns[pair]), x[now, pl.ds(base, PAIR), :])

    def step(index, carry):
        now = lax.rem(index, 2)
        after = 1 - now

        def inner_gram(pair, carry):
            take_gram(pair, now)
            return carry

        lax.fori_loop(1, last, inner_gram, 0)
        @pl.when(index > 0)
        def _():
            wait_edges(now)

        def edge_gram(which, carry):
            take_gram(which * last, now)
            return carry

        lax.fori_loop(0, 2, edge_gram, 0)

        @pl.when(me < pairs)
        def _():
            own()

        @pl.when(jnp.logical_and(index > 0, has_left))
        def _():
            edge_left(after).wait_send()

        take_turn(0)
        turned = apply(0, now)
        x[after, pl.ds(pl.multiple_of(jnp.where(has_left, PAIR, 0), BLOCK), BLOCK), :] = turned[:BLOCK]

        @pl.when(has_left)
        def _():
            edges[0] = turned[BLOCK:]
            edge_left(after).start()

        @pl.when(jnp.logical_not(has_left))
        def _():
            x[after, pl.ds(PAIR, BLOCK), :] = turned[BLOCK:]

        @pl.when(jnp.logical_and(index > 0, has_right))
        def _():
            edge_right(after).wait_send()

        take_turn(last)
        turned_last = apply(last, now)
        x[after, pl.ds((last - 1) * PAIR + BLOCK, BLOCK), :] = turned_last[BLOCK:]

        @pl.when(has_right)
        def _():
            edges[1] = turned_last[:BLOCK]
            edge_right(after).start()

        @pl.when(jnp.logical_not(has_right))
        def _():
            x[after, pl.ds(last * PAIR + BLOCK, BLOCK), :] = turned_last[:BLOCK]

        def inner_apply(pair, carry):
            take_turn(pair)
            turned = apply(pair, now)
            x[after, pl.ds(pl.multiple_of((pair + 1) * PAIR, PAIR), BLOCK), :] = turned[:BLOCK]
            x[after, pl.ds(pl.multiple_of((pair - 1) * PAIR + BLOCK, BLOCK), BLOCK), :] = turned[BLOCK:]
            return carry

        lax.fori_loop(1, last, inner_apply, 0)

        def settle(pair, carry):
            @pl.when(pair != me)
            def _():
                gram_copy(pair).wait_send()

                @pl.when(lax.rem(pair, 2) == core)
                def _():
                    pass_copy(pair).wait_send()
            return carry

        lax.fori_loop(0, pairs, settle, 0)

        @pl.when(me < pairs)
        def _():
            def settle_turn(other, carry):
                turn_copy(other).wait_send()
                return carry

            lax.fori_loop(0, rows // 2, settle_turn, 0)

        return carry

    lax.fori_loop(0, STEPS, step, 0)
    final = STEPS % 2

    def out_copy(start, size, which):
        return pltpu.make_async_copy(
            x.at[final, pl.ds(start, size)], out_ref.at[pl.ds(start, size)], out_sem.at[which]
        )

    middle = out_copy(BLOCK, width - PAIR, 0)
    middle.start()
    wait_edges(final)
    first = out_copy(0, BLOCK, 1)
    first.start()
    ending = out_copy(width - BLOCK, BLOCK, 2)
    ending.start()

    @pl.when(has_left)
    def _():
        edge_left(final).wait_send()

    @pl.when(has_right)
    def _():
        edge_right(final).wait_send()

    middle.wait()
    first.wait()
    ending.wait()


def solution(mesh):
    rows, cols = mesh.shape["row"], mesh.shape["col"]

    def local(columns, block_order):
        width, length = columns.shape
        pairs = width // PAIR
        assert 3 <= pairs <= rows and rows % 2 == 0
        dma = pltpu.SemaphoreType.DMA
        return pl.pallas_call(
            functools.partial(kernel, rows, cols, pairs),
            out_shape=jax.ShapeDtypeStruct((width, length), jnp.float32),
            in_specs=[pl.BlockSpec(memory_space=pltpu.SMEM), pl.BlockSpec(memory_space=pltpu.VMEM)],
            out_specs=pl.BlockSpec(memory_space=pl.ANY),
            scratch_shapes=[
                pltpu.VMEM((2, width, length), jnp.float32),
                pltpu.VMEM((pairs, PACKED, PAIR), jnp.float32),
                pltpu.VMEM((rows, PACKED, PAIR), jnp.float32),
                pltpu.VMEM((pairs, BLOCK + 8, PAIR), jnp.float32),
                pltpu.VMEM((2, BLOCK, length), jnp.float32),
                dma((pairs,)),
                dma((rows,)),
                dma((rows // 2,)),
                dma((pairs,)),
                dma((pairs,)),
                dma((2,)),
                dma((2, 2)),
                dma((3,)),
            ],
            compiler_params=pltpu.CompilerParams(
                collective_id=0, has_side_effects=True, vmem_limit_bytes=56 * 1024 * 1024
            ),
        )(block_order, columns.reshape(2 * pairs, BLOCK, length))

    placed = (P("col", "row"), P("col"))
    return jax.shard_map(local, mesh=mesh, in_specs=placed, out_specs=P("col", "row"), check_vma=False)
```
